32 devices in a mesh: bl: 8 (over z, x), tm: 4 (over y, core).
Axes of the slice: x: 2, y: 2, z: 4, core: 2. Of those that a mesh axis runs over, the one named last changes fastest.
Arguments:
- visibility_real: bfloat16 [3072, 16, 1024], P('bl', 'tm'), may hold values from -6 to 6
- visibility_imag: bfloat16 [3072, 16, 1024], P('bl', 'tm'), may hold values from -6 to 6
- weights: int32 [3072, 16], P('bl', 'tm'), may hold values from 0 to 8
- labels: int32 [3072], P('bl'), may hold values from 0 to 511, as said below
- owner_of: int32 [512], replicated, may hold values from 0 to 7, as said below
Outputs:
- bandpower: float32 [512, 1024], P(('bl', 'tm'))
The draws below stay inside these ranges and needn't reach their ends.
Inputs may be any that keep to these rules, and one draw needn't show every extreme that they name: Of the rows of one device, at most 72 have labels of groups with one owner, and these carry at most 18 different labels; in every draw some owner gets exactly 72 such rows with exactly 18 labels from every device. `owner_of`: every owner owns exactly 64 groups.
All inputs are finite; a program needn't handle non-finite values.
Results may differ from the reference program's by a relative error of at most 0.0003.
Values may be sent and summed in bfloat16 or wider, within the bound.
A program may use at most 128 MiB of HBM per device.

```python
import math
import jax
import jax.numpy as jnp
from jax import lax

FREQ_CHANNELS = 1024
B_DEV = 384
G_DEV = 64
BASELINE_COUNT = 3072
TIME_STEPS = 16
CAP = 72
KEYS = 18
N_BL = 8


def layout_plan(key):
    groups = G_DEV * N_BL
    group_order = jax.random.permutation(jax.random.fold_in(key, 101), groups).astype(jnp.int32)
    owner_of = jnp.zeros((groups,), jnp.int32).at[group_order].set(jnp.arange(groups, dtype=jnp.int32) // G_DEV)
    heaviest_owner = jax.random.randint(jax.random.fold_in(key, 102), (), 0, N_BL)

    def one_device(device):
        device_key = jax.random.fold_in(jax.random.fold_in(key, 103), device)
        slot_ids = jnp.arange(N_BL * CAP, dtype=jnp.int32)
        priority = jax.random.permutation(jax.random.fold_in(device_key, 1), N_BL * CAP).astype(jnp.int32)
        priority = jnp.where(slot_ids // CAP == heaviest_owner, priority - N_BL * CAP, priority)
        chosen = jnp.argsort(priority)[:B_DEV].astype(jnp.int32)
        target = chosen // CAP
        within = chosen % CAP

        def candidates(owner):
            owner_key = jax.random.fold_in(jax.random.fold_in(device_key, 2), owner)
            return jax.random.permutation(owner_key, G_DEV)[:KEYS].astype(jnp.int32)
        offsets = jax.vmap(candidates)(jnp.arange(N_BL, dtype=jnp.int32))
        picked = offsets[target, within % KEYS]
        row_label = group_order[target * G_DEV + picked]
        shuffle = jax.random.permutation(jax.random.fold_in(device_key, 3), B_DEV)
        return row_label[shuffle]
    labels = jax.vmap(one_device)(jnp.arange(N_BL, dtype=jnp.int32)).reshape(-1)
    return (labels.astype(jnp.int32), owner_of)


def draw_labels(key, part):
    return layout_plan(key)[0]


def draw_owner_of(key, part):
    return layout_plan(key)[1]


def set_ends(values, stream_key, low, top_value):
    dims = values.shape
    index_at = [jax.random.randint(jax.random.fold_in(stream_key, axis), (), 0, dims[axis]) for axis in range(len(dims))]
    values = values.at[tuple(index_at)].set(low)
    longest = dims.index(max(dims))
    index_at[longest] = (index_at[longest] + 1) % dims[longest]
    return values.at[tuple(index_at)].set(top_value)


def shard_levels(key, dims, split, smallest, largest):
    loudness = 1.0
    for dim, blocks in split:
        draws = jax.random.uniform(jax.random.fold_in(jax.random.fold_in(key, 6), dim), (blocks,), jnp.float32, smallest / len(split), largest / len(split))
        loudness = loudness * jnp.repeat(jnp.exp(draws), dims[dim] // blocks).reshape((-1,) + (1,) * (len(dims) - 1 - dim))
    return loudness


def noise(key, shape, width, reach, shards=(), kind=jnp.bfloat16):
    level = shard_levels(key, shape, shards, -0.22, 0.18) if shards else 1.0
    array = jax.random.normal(key, shape, jnp.float32) * width * level
    return jnp.minimum(jnp.maximum(array, -reach), reach).astype(kind)


def setup_inputs(seed: int = 0) -> dict:
    keys = jax.random.split(jax.random.key(seed), 6)
    return {
        "visibility_real": noise(keys[0], (BASELINE_COUNT, TIME_STEPS, FREQ_CHANNELS), 1.0, 6.0, ((0, 8), (1, 4))),
        "visibility_imag": noise(keys[1], (BASELINE_COUNT, TIME_STEPS, FREQ_CHANNELS), 1.0, 6.0, ((0, 8), (1, 4))),
        "weights": set_ends(jax.random.randint(keys[2], (BASELINE_COUNT, TIME_STEPS), 0, 9), jax.random.fold_in(keys[2], 1), 0, 8).astype(jnp.int32),
        "labels": draw_labels(jax.random.fold_in(keys[5], 71), 0),
        "owner_of": draw_owner_of(jax.random.fold_in(keys[5], 71), 0),
    }


HARRIS = (0.35875, 0.48829, 0.14128, 0.01168)

def taper_of(length):
    phase_angle = 2.0 * math.pi / length * jnp.arange(length, dtype=jnp.float32)
    return HARRIS[0] - HARRIS[1] * jnp.cos(phase_angle) + HARRIS[2] * jnp.cos(2.0 * phase_angle) - HARRIS[3] * jnp.cos(3.0 * phase_angle)

def reference(visibility_real, visibility_imag, weights, labels, owner_of):
    groups = owner_of.shape[0]
    channels = visibility_real.shape[2]
    times = visibility_real.shape[1]
    window_taper = taper_of(channels)
    window_taper = window_taper / jnp.sqrt(jnp.sum(window_taper * window_taper))

    def advance(carried, instant):
        prior_real, prior_imag, running = carried
        row_weight = lax.dynamic_index_in_dim(weights, instant, 1, keepdims=False).astype(jnp.float32)
        slab_real = lax.dynamic_index_in_dim(visibility_real, instant, 1, keepdims=False).astype(jnp.float32)
        slab_imag = lax.dynamic_index_in_dim(visibility_imag, instant, 1, keepdims=False).astype(jnp.float32)
        sum_real = jax.ops.segment_sum(row_weight[:, None] * slab_real, labels, num_segments=groups)
        sum_imag = jax.ops.segment_sum(row_weight[:, None] * slab_imag, labels, num_segments=groups)
        weight_sum = jax.ops.segment_sum(row_weight, labels, num_segments=groups)
        divisor = jnp.maximum(weight_sum, 1.0)[:, None]
        mean_real = sum_real / divisor
        mean_imag = sum_imag / divisor
        spectrum = jnp.fft.fft((mean_real + 1j * mean_imag) * window_taper[None, :], axis=1)
        spec_real = jnp.real(spectrum)
        spec_imag = jnp.imag(spectrum)
        cross = prior_real * spec_real + prior_imag * spec_imag
        running = running + jnp.where(instant > 0, cross, jnp.zeros_like(cross))
        return ((spec_real, spec_imag, running), instant)
    zeros = jnp.zeros((groups, channels), jnp.float32)
    final_state, unused = lax.scan(advance, (zeros, zeros, zeros), jnp.arange(times, dtype=jnp.int32))
    order = jnp.argsort(owner_of * groups + jnp.arange(groups, dtype=jnp.int32))
    return final_state[2][order]
```

```python
import math

import jax
import jax.numpy as jnp
from jax import lax
from jax.sharding import PartitionSpec as P

HARRIS = (0.35875, 0.48829, 0.14128, 0.01168)
RADIX = 4


def taper_of(length):
    phase_angle = 2.0 * math.pi / length * jnp.arange(length, dtype=jnp.float32)
    taper = (
        HARRIS[0]
        - HARRIS[1] * jnp.cos(phase_angle)
        + HARRIS[2] * jnp.cos(2.0 * phase_angle)
        - HARRIS[3] * jnp.cos(3.0 * phase_angle)
    )
    return taper / jnp.sqrt(jnp.sum(taper * taper))


def dft_table(channels):
    short = channels // RADIX
    residue = jnp.arange(RADIX, dtype=jnp.int32)[:, None, None]
    row = jnp.arange(short, dtype=jnp.int32)[None, :, None]
    column = jnp.arange(short, dtype=jnp.int32)[None, None, :]
    turns = row * (RADIX * column + residue) % channels
    angle = 2.0 * math.pi / channels * turns.astype(jnp.float32)
    cosine, sine = jnp.cos(angle), jnp.sin(angle)
    top = jnp.concatenate([cosine, -sine], axis=2)
    bottom = jnp.concatenate([sine, cosine], axis=2)
    return jnp.concatenate([top, bottom], axis=1)


def owner_rank(owner_of, owners):
    hits = (owner_of[:, None] == jnp.arange(owners, dtype=jnp.int32)[None, :]).astype(jnp.int32)
    earlier = jnp.cumsum(hits, axis=0) - hits
    return jnp.sum(earlier * hits, axis=1)


def slots(labels, owner_of, owners, distinct):
    groups = owner_of.shape[0]
    per_owner = groups // owners
    group_rank = owner_rank(owner_of, owners)
    label_match = labels[:, None] == jnp.arange(groups, dtype=jnp.int32)[None, :]
    group_key = owner_of * per_owner + group_rank
    local_key = jnp.sum(jnp.where(label_match, group_key[None, :], 0), axis=1)
    key_match = local_key[:, None] == jnp.arange(groups, dtype=jnp.int32)[None, :]
    present = jnp.any(key_match, axis=0).astype(jnp.int32).reshape(owners, per_owner)
    order_within = jnp.cumsum(present, axis=1) - present
    slot_of_key = (jnp.arange(owners, dtype=jnp.int32)[:, None] * distinct + order_within).reshape(
        groups
    )
    row_slot = jnp.sum(jnp.where(key_match, slot_of_key[None, :], 0), axis=1)
    slot_hit = (
        order_within[:, :, None] == jnp.arange(distinct, dtype=jnp.int32)[None, None, :]
    ) & (present[:, :, None] > 0)
    slot_rank = jnp.sum(
        jnp.where(slot_hit, jnp.arange(per_owner, dtype=jnp.int32)[None, :, None], 0), axis=1
    )
    return row_slot, slot_rank


def per_device(visibility_real, visibility_imag, weights, labels, owner_of):
    row_count, times, channels = visibility_real.shape
    owners = lax.axis_size("bl")
    parts = lax.axis_size("tm")
    groups = owner_of.shape[0]
    per_owner = groups // owners
    capacity = 3 * row_count // (2 * owners)
    distinct = min(capacity // 4, per_owner // 2)
    row_slot, slot_rank = slots(labels, owner_of, owners, distinct)

    sent = distinct * times
    slot_id = jnp.arange(owners * distinct, dtype=jnp.int32)
    same_time = jnp.eye(times, dtype=jnp.int32)
    hit = (row_slot[None, :] == slot_id[:, None]).astype(jnp.int32)
    folder = (
        (hit[:, None, :, None] * (same_time[:, None, :] * weights[None])[None])
        .astype(jnp.bfloat16)
        .reshape(owners * sent, row_count * times)
    )
    part_weight = jnp.sum(hit[:, :, None] * weights[None], axis=1).astype(jnp.float32)
    part_real = jnp.dot(
        folder,
        visibility_real.reshape(row_count * times, channels),
        preferred_element_type=jnp.float32,
    )
    part_imag = jnp.dot(
        folder,
        visibility_imag.reshape(row_count * times, channels),
        preferred_element_type=jnp.float32,
    )
    peak = jnp.maximum(
        jnp.max(jnp.abs(part_real), axis=1), jnp.max(jnp.abs(part_imag), axis=1)
    )
    step = lax.reduce_precision(jnp.maximum(peak, 1e-30) * (1.0078125 / 32767.0), 8, 7)
    invert = (1.0 / step)[:, None]
    code_real = jnp.round(part_real * invert).astype(jnp.int32)
    code_imag = jnp.round(part_imag * invert).astype(jnp.int32)
    packed = ((code_real << 16) | (code_imag & 65535)).reshape(owners, sent, channels)
    rank_row = jnp.broadcast_to(slot_rank[:, :, None], (owners, distinct, times))
    note = jnp.stack(
        [
            step.reshape(owners, sent),
            part_weight.reshape(owners, sent),
            rank_row.reshape(owners, sent).astype(jnp.float32),
        ],
        axis=1,
    )
    came_note = lax.all_to_all(note, "bl", split_axis=0, concat_axis=0, tiled=True)
    came = lax.all_to_all(packed, "bl", split_axis=0, concat_axis=0, tiled=True)

    came_step = came_note[:, 0].reshape(owners, distinct, times)
    came_weight = came_note[:, 1].reshape(owners, distinct, times)
    came_rank = came_note[:, 2].reshape(owners, distinct, times).astype(jnp.int32)
    time_id = jnp.arange(times, dtype=jnp.int32)
    group_id = jnp.arange(per_owner, dtype=jnp.int32)
    chosen = (came_rank[None, None] == group_id[None, :, None, None, None]) & (
        time_id[:, None, None, None, None] == time_id[None, None, None, None, :]
    )
    selector = (
        jnp.where(chosen, came_step[None, None], 0.0)
        .astype(jnp.bfloat16)
        .reshape(times * per_owner, owners * sent)
    )
    weight_sum = jnp.sum(jnp.where(chosen, came_weight[None, None], 0.0), axis=(2, 3, 4))
    scale = (1.0 / jnp.maximum(weight_sum, 1.0)).reshape(times * per_owner, 1)

    came = came.reshape(owners * sent, channels)
    real_high = (came >> 24).astype(jnp.bfloat16)
    real_low = ((came >> 16) & 255).astype(jnp.bfloat16)
    imag_code = (came << 16) >> 16
    imag_high = (imag_code >> 8).astype(jnp.bfloat16)
    imag_low = (imag_code & 255).astype(jnp.bfloat16)

    def gather(high, low):
        upper = jnp.dot(selector, high, preferred_element_type=jnp.float32)
        lower = jnp.dot(selector, low, preferred_element_type=jnp.float32)
        return 256.0 * upper + lower

    taper = taper_of(channels)[None, :]
    mean_real = gather(real_high, real_low) * scale * taper
    mean_imag = gather(imag_high, imag_low) * scale * taper
    short = channels // RADIX
    r = [mean_real[:, i * short : (i + 1) * short] for i in range(RADIX)]
    m = [mean_imag[:, i * short : (i + 1) * short] for i in range(RADIX)]
    er, ei, fr, fi = r[0] + r[2], m[0] + m[2], r[1] + r[3], m[1] + m[3]
    gr, gi, hr, hi = r[0] - r[2], m[0] - m[2], r[1] - r[3], m[1] - m[3]
    folded = jnp.stack(
        [
            jnp.concatenate([er + fr, ei + fi], axis=1),
            jnp.concatenate([gr + hi, gi - hr], axis=1),
            jnp.concatenate([er - fr, ei - fi], axis=1),
            jnp.concatenate([gr - hi, gi + hr], axis=1),
        ]
    )
    spectrum = jnp.einsum(
        "qnf,qfk->qnk", folded, dft_table(channels), precision=lax.Precision.HIGH
    ).reshape(RADIX, times, per_owner, 2 * short)
    size = lax.axis_size("tm")
    following = lax.ppermute(spectrum[:, 0], "tm", [(i, i - 1) for i in range(1, size)])
    pair = jnp.sum(spectrum[:, :-1] * spectrum[:, 1:], axis=1) + spectrum[:, -1] * following
    power = pair[..., :short] + pair[..., short:]
    rows = per_owner // parts
    power = power.reshape(RADIX, parts, rows, short).transpose(1, 2, 0, 3)
    me = lax.axis_index("tm")
    total = lax.dynamic_index_in_dim(power, me, 0, keepdims=False)
    for hop in range(1, parts):
        block = lax.dynamic_index_in_dim(power, lax.rem(me + hop, parts), 0, keepdims=False)
        route = [(i, (i + hop) % parts) for i in range(parts)]
        total = total + lax.ppermute(block, "tm", route)
    return total.transpose(0, 2, 1).reshape(rows, channels)


def solution(mesh):
    placed = (P("bl", "tm", None), P("bl", "tm", None), P("bl", "tm"), P("bl"), P())
    return jax.shard_map(
        per_device, mesh=mesh, in_specs=placed, out_specs=P(("bl", "tm"), None), check_vma=False
    )
```

```python
import math

import jax
import jax.numpy as jnp
from jax import lax
from jax.sharding import PartitionSpec as P

HARRIS = (0.35875, 0.48829, 0.14128, 0.01168)
RADIX = 4


def taper_of(length):
    phase_angle = 2.0 * math.pi / length * jnp.arange(length, dtype=jnp.float32)
    taper = (
        HARRIS[0]
        - HARRIS[1] * jnp.cos(phase_angle)
        + HARRIS[2] * jnp.cos(2.0 * phase_angle)
        - HARRIS[3] * jnp.cos(3.0 * phase_angle)
    )
    return taper / jnp.sqrt(jnp.sum(taper * taper))


def dft_table(channels):
    short = channels // RADIX
    fine = math.isqrt(short)
    turn = 2.0 * math.pi / channels
    delay = (
        RADIX * jnp.arange(short, dtype=jnp.int32)[None, None, :]
        + jnp.arange(RADIX, dtype=jnp.int32)[:, None, None]
    )

    def wave(rows):
        angle = turn * (rows[None, :, None] * delay % channels).astype(jnp.float32)
        return lax.optimization_barrier((jnp.cos(angle), jnp.sin(angle)))

    coarse_cos, coarse_sin = wave(fine * jnp.arange(short // fine, dtype=jnp.int32))
    fine_cos, fine_sin = wave(jnp.arange(fine, dtype=jnp.int32))
    ac, as_ = coarse_cos[:, :, None, :], coarse_sin[:, :, None, :]
    bc, bs = fine_cos[:, None], fine_sin[:, None]
    cosine = (ac * bc - as_ * bs).reshape(RADIX, short, short)
    sine = (as_ * bc + ac * bs).reshape(RADIX, short, short)
    top = jnp.concatenate([cosine, -sine], axis=2)
    bottom = jnp.concatenate([sine, cosine], axis=2)
    return jnp.concatenate([top, bottom], axis=1)


def owner_rank(owner_of, owners):
    hits = (owner_of[:, None] == jnp.arange(owners, dtype=jnp.int32)[None, :]).astype(jnp.int32)
    earlier = jnp.cumsum(hits, axis=0) - hits
    return jnp.sum(earlier * hits, axis=1)


def slots(labels, owner_of, owners, distinct):
    groups = owner_of.shape[0]
    per_owner = groups // owners
    group_rank = owner_rank(owner_of, owners)
    label_match = labels[:, None] == jnp.arange(groups, dtype=jnp.int32)[None, :]
    group_key = owner_of * per_owner + group_rank
    local_key = jnp.sum(jnp.where(label_match, group_key[None, :], 0), axis=1)
    key_match = local_key[:, None] == jnp.arange(groups, dtype=jnp.int32)[None, :]
    present = jnp.any(key_match, axis=0).astype(jnp.int32).reshape(owners, per_owner)
    order_within = jnp.cumsum(present, axis=1) - present
    slot_of_key = (jnp.arange(owners, dtype=jnp.int32)[:, None] * distinct + order_within).reshape(
        groups
    )
    row_slot = jnp.sum(jnp.where(key_match, slot_of_key[None, :], 0), axis=1)
    slot_hit = (
        order_within[:, :, None] == jnp.arange(distinct, dtype=jnp.int32)[None, None, :]
    ) & (present[:, :, None] > 0)
    slot_rank = jnp.sum(
        jnp.where(slot_hit, jnp.arange(per_owner, dtype=jnp.int32)[None, :, None], 0), axis=1
    )
    return row_slot, slot_rank


def per_device(visibility_real, visibility_imag, weights, labels, owner_of):
    row_count, times, channels = visibility_real.shape
    owners = lax.axis_size("bl")
    parts = lax.axis_size("tm")
    groups = owner_of.shape[0]
    per_owner = groups // owners
    capacity = 3 * row_count // (2 * owners)
    distinct = min(capacity // 4, per_owner // 2)
    row_slot, slot_rank = slots(labels, owner_of, owners, distinct)

    sent = distinct * times
    slot_id = jnp.arange(owners * sent, dtype=jnp.int32)[:, None]
    row_key = row_slot[:, None] * times + jnp.arange(times, dtype=jnp.int32)[None, :]
    row_key = row_key.reshape(1, row_count * times)
    row_weight = weights.astype(jnp.float32).reshape(1, row_count * times)
    folder = jnp.where(slot_id == row_key, row_weight, 0.0)
    part_weight = jnp.sum(folder, axis=1)
    folder = folder.astype(jnp.bfloat16)
    part_real = jnp.dot(
        folder,
        visibility_real.reshape(row_count * times, channels),
        preferred_element_type=jnp.float32,
    )
    part_imag = jnp.dot(
        folder,
        visibility_imag.reshape(row_count * times, channels),
        preferred_element_type=jnp.float32,
    )
    peak = jnp.maximum(
        jnp.max(jnp.abs(part_real), axis=1), jnp.max(jnp.abs(part_imag), axis=1)
    )
    step = lax.reduce_precision(jnp.maximum(peak, 1e-30) * (1.0078125 / 32767.0), 8, 7)
    invert = (1.0 / step)[:, None]
    code_real = jnp.round(part_real * invert).astype(jnp.int32)
    code_imag = jnp.round(part_imag * invert).astype(jnp.int32)
    packed = ((code_real << 16) | (code_imag & 65535)).reshape(owners, sent, channels)
    rank_row = jnp.broadcast_to(slot_rank[:, :, None], (owners, distinct, times))
    note = jnp.stack(
        [
            step.reshape(owners, sent),
            part_weight.reshape(owners, sent),
            rank_row.reshape(owners, sent).astype(jnp.float32),
        ],
        axis=1,
    )
    came_note = lax.all_to_all(note, "bl", split_axis=0, concat_axis=0, tiled=True)
    came = lax.all_to_all(packed, "bl", split_axis=0, concat_axis=0, tiled=True)

    came_step = came_note[:, 0].reshape(1, owners * sent)
    came_weight = came_note[:, 1].reshape(1, owners * sent)
    came_rank = came_note[:, 2].reshape(1, owners * sent).astype(jnp.int32)
    came_time = jnp.arange(owners * sent, dtype=jnp.int32)[None, :] % times
    item = jnp.arange(times * per_owner, dtype=jnp.int32)[:, None]
    chosen = item == came_time * per_owner + came_rank
    selector = jnp.where(chosen, came_step, 0.0).astype(jnp.bfloat16)
    weight_sum = jnp.sum(jnp.where(chosen, came_weight, 0.0), axis=1)
    scale = (1.0 / jnp.maximum(weight_sum, 1.0)).reshape(times * per_owner, 1)

    came = came.reshape(owners * sent, channels)
    real_high = (came >> 24).astype(jnp.bfloat16)
    real_low = ((came >> 16) & 255).astype(jnp.bfloat16)
    imag_code = (came << 16) >> 16
    imag_high = (imag_code >> 8).astype(jnp.bfloat16)
    imag_low = (imag_code & 255).astype(jnp.bfloat16)

    def gather(high, low):
        upper = jnp.dot(selector, high, preferred_element_type=jnp.float32)
        lower = jnp.dot(selector, low, preferred_element_type=jnp.float32)
        return 256.0 * upper + lower

    taper = taper_of(channels)[None, :]
    mean_real = gather(real_high, real_low) * scale * taper
    mean_imag = gather(imag_high, imag_low) * scale * taper
    short = channels // RADIX
    r = [mean_real[:, i * short : (i + 1) * short] for i in range(RADIX)]
    m = [mean_imag[:, i * short : (i + 1) * short] for i in range(RADIX)]
    er, ei, fr, fi = r[0] + r[2], m[0] + m[2], r[1] + r[3], m[1] + m[3]
    gr, gi, hr, hi = r[0] - r[2], m[0] - m[2], r[1] - r[3], m[1] - m[3]
    folded = jnp.stack(
        [
            jnp.concatenate([er + fr, ei + fi], axis=1),
            jnp.concatenate([gr + hi, gi - hr], axis=1),
            jnp.concatenate([er - fr, ei - fi], axis=1),
            jnp.concatenate([gr - hi, gi + hr], axis=1),
        ]
    )
    spectrum = jnp.einsum(
        "qnf,qfk->qnk", folded, dft_table(channels), precision=lax.Precision.HIGH
    ).reshape(RADIX, times, per_owner, 2 * short)
    size = lax.axis_size("tm")
    following = lax.ppermute(spectrum[:, 0], "tm", [(i, i - 1) for i in range(1, size)])
    pair = jnp.sum(spectrum[:, :-1] * spectrum[:, 1:], axis=1) + spectrum[:, -1] * following
    power = pair[..., :short] + pair[..., short:]
    rows = per_owner // parts
    power = power.reshape(RADIX, parts, rows, short).transpose(1, 2, 0, 3)
    me = lax.axis_index("tm")
    total = lax.dynamic_index_in_dim(power, me, 0, keepdims=False)
    for hop in range(1, parts):
        block = lax.dynamic_index_in_dim(power, lax.rem(me + hop, parts), 0, keepdims=False)
        route = [(i, (i + hop) % parts) for i in range(parts)]
        total = total + lax.ppermute(block, "tm", route)
    return total.transpose(0, 2, 1).reshape(rows, channels)


def solution(mesh):
    placed = (P("bl", "tm", None), P("bl", "tm", None), P("bl", "tm"), P("bl"), P())
    return jax.shard_map(
        per_device, mesh=mesh, in_specs=placed, out_specs=P(("bl", "tm"), None), check_vma=False
    )
```

```python
import functools
import math

import jax
import jax.numpy as jnp
from jax import lax
from jax.experimental import pallas as pl
from jax.experimental.pallas import tpu as pltpu
from jax.sharding import PartitionSpec as P

HARRIS = (0.35875, 0.48829, 0.14128, 0.01168)
RADIX = 4


def taper_of(length):
    phase_angle = 2.0 * math.pi / length * jnp.arange(length, dtype=jnp.float32)
    taper = (
        HARRIS[0]
        - HARRIS[1] * jnp.cos(phase_angle)
        + HARRIS[2] * jnp.cos(2.0 * phase_angle)
        - HARRIS[3] * jnp.cos(3.0 * phase_angle)
    )
    return taper / jnp.sqrt(jnp.sum(taper * taper))


def dft_table(channels):
    short = channels // RADIX
    fine = math.isqrt(short)
    turn = 2.0 * math.pi / channels
    delay = (
        RADIX * jnp.arange(short, dtype=jnp.int32)[None, None, :]
        + jnp.arange(RADIX, dtype=jnp.int32)[:, None, None]
    )

    def wave(rows):
        angle = turn * (rows[None, :, None] * delay % channels).astype(jnp.float32)
        return lax.optimization_barrier((jnp.cos(angle), jnp.sin(angle)))

    coarse_cos, coarse_sin = wave(fine * jnp.arange(short // fine, dtype=jnp.int32))
    fine_cos, fine_sin = wave(jnp.arange(fine, dtype=jnp.int32))
    ac, as_ = coarse_cos[:, :, None, :], coarse_sin[:, :, None, :]
    bc, bs = fine_cos[:, None], fine_sin[:, None]
    cosine = (ac * bc - as_ * bs).reshape(RADIX, short, short)
    sine = (as_ * bc + ac * bs).reshape(RADIX, short, short)
    top = jnp.concatenate([cosine, -sine], axis=2)
    bottom = jnp.concatenate([sine, cosine], axis=2)
    return jnp.concatenate([top, bottom], axis=1)


def owner_rank(owner_of, owners):
    hits = (owner_of[:, None] == jnp.arange(owners, dtype=jnp.int32)[None, :]).astype(jnp.int32)
    earlier = jnp.cumsum(hits, axis=0) - hits
    return jnp.sum(earlier * hits, axis=1)


def slots(labels, owner_of, owners, distinct):
    groups = owner_of.shape[0]
    per_owner = groups // owners
    group_rank = owner_rank(owner_of, owners)
    label_match = labels[:, None] == jnp.arange(groups, dtype=jnp.int32)[None, :]
    group_key = owner_of * per_owner + group_rank
    local_key = jnp.sum(jnp.where(label_match, group_key[None, :], 0), axis=1)
    key_match = local_key[:, None] == jnp.arange(groups, dtype=jnp.int32)[None, :]
    present = jnp.any(key_match, axis=0).astype(jnp.int32).reshape(owners, per_owner)
    order_within = jnp.cumsum(present, axis=1) - present
    slot_of_key = (jnp.arange(owners, dtype=jnp.int32)[:, None] * distinct + order_within).reshape(
        groups
    )
    row_slot = jnp.sum(jnp.where(key_match, slot_of_key[None, :], 0), axis=1)
    slot_hit = (
        order_within[:, :, None] == jnp.arange(distinct, dtype=jnp.int32)[None, None, :]
    ) & (present[:, :, None] > 0)
    slot_rank = jnp.sum(
        jnp.where(slot_hit, jnp.arange(per_owner, dtype=jnp.int32)[None, :, None], 0), axis=1
    )
    return row_slot, slot_rank


def greet(axis, size):
    me = lax.axis_index(axis)
    barrier = pltpu.get_barrier_semaphore()
    for hop in range(1, size):
        pl.semaphore_signal(
            barrier,
            inc=1,
            device_id={axis: lax.rem(me + hop, size)},
            device_id_type=pl.DeviceIdType.MESH,
        )
    pl.semaphore_wait(barrier, size - 1)
    return me


def exchange_kernel(size, data, note, data_out, note_out, held, kept, sends, arrivals, local):
    me = greet("bl", size)
    copies = []
    for which, (source, target) in enumerate(((note, note_out), (data, data_out))):
        for hop in range(1, size):
            peer = lax.rem(me + hop, size)
            copy = pltpu.make_async_remote_copy(
                src_ref=source.at[peer],
                dst_ref=target.at[me],
                send_sem=sends.at[which, hop - 1],
                recv_sem=arrivals.at[which, hop - 1],
                device_id={"bl": peer},
                device_id_type=pl.DeviceIdType.MESH,
            )
            copy.start()
            copies.append(copy)
    inward = [
        pltpu.make_async_copy(data.at[me], held, local.at[0]),
        pltpu.make_async_copy(note.at[me], kept, local.at[1]),
    ]
    outward = [
        pltpu.make_async_copy(held, data_out.at[me], local.at[0]),
        pltpu.make_async_copy(kept, note_out.at[me], local.at[1]),
    ]
    for copy in inward:
        copy.start()
    for copy in inward:
        copy.wait()
    for copy in outward:
        copy.start()
    for copy in outward:
        copy.wait()
    for copy in copies:
        copy.wait()


def exchange(data, note):
    size = data.shape[0]
    anywhere = pl.BlockSpec(memory_space=pl.ANY)
    return pl.pallas_call(
        functools.partial(exchange_kernel, size),
        out_shape=[
            jax.ShapeDtypeStruct(data.shape, data.dtype),
            jax.ShapeDtypeStruct(note.shape, note.dtype),
        ],
        in_specs=[anywhere, anywhere],
        out_specs=[anywhere, anywhere],
        scratch_shapes=[
            pltpu.VMEM(data.shape[1:], data.dtype),
            pltpu.VMEM(note.shape[1:], note.dtype),
            pltpu.SemaphoreType.DMA((2, size - 1)),
            pltpu.SemaphoreType.DMA((2, size - 1)),
            pltpu.SemaphoreType.DMA((2,)),
        ],
        compiler_params=pltpu.CompilerParams(collective_id=0, has_side_effects=True),
        cost_estimate=pl.CostEstimate(
            flops=0, bytes_accessed=32 * data.size, transcendentals=0
        ),
    )(data, note)


def tail_kernel(size, spectrum, out, following, share, came, sends, arrivals, step_sems):
    radix, times, groups, width = spectrum.shape
    short = width // 2
    rows = groups // size
    me = greet("tm", size)
    ahead = pltpu.make_async_remote_copy(
        src_ref=spectrum.at[:, 0],
        dst_ref=following,
        send_sem=step_sems.at[0],
        recv_sem=step_sems.at[1],
        device_id={"tm": lax.rem(me + size - 1, size)},
        device_id_type=pl.DeviceIdType.MESH,
    )
    ahead.start()
    for q in range(radix):
        pair = spectrum[q, 0] * spectrum[q, 1]
        for t in range(1, times - 1):
            pair += spectrum[q, t] * spectrum[q, t + 1]
        power = pair[:, :short] + pair[:, short:]
        for p in range(size):
            share[p, q] = power[p * rows : (p + 1) * rows]
    ahead.wait()
    for q in range(radix):
        pair = spectrum[q, times - 1] * following[q]
        power = pair[:, :short] + pair[:, short:]
        power = jnp.where(me < size - 1, power, 0.0)
        for p in range(size):
            share[p, q] += power[p * rows : (p + 1) * rows]
    copies = []
    for hop in range(1, size):
        peer = lax.rem(me + hop, size)
        copy = pltpu.make_async_remote_copy(
            src_ref=share.at[peer],
            dst_ref=came.at[hop - 1],
            send_sem=sends.at[hop - 1],
            recv_sem=arrivals.at[hop - 1],
            device_id={"tm": peer},
            device_id_type=pl.DeviceIdType.MESH,
        )
        copy.start()
        copies.append(copy)
    total = share[me]
    for hop, copy in enumerate(copies):
        copy.wait()
        total += came[hop]
    out[...] = total


def tail(spectrum, size):
    radix, times, groups, width = spectrum.shape
    block = (radix, groups // size, width // 2)
    inside = pl.BlockSpec(memory_space=pltpu.VMEM)
    return pl.pallas_call(
        functools.partial(tail_kernel, size),
        out_shape=jax.ShapeDtypeStruct(block, jnp.float32),
        in_specs=[inside],
        out_specs=inside,
        scratch_shapes=[
            pltpu.VMEM((radix, groups, width), jnp.float32),
            pltpu.VMEM((size,) + block, jnp.float32),
            pltpu.VMEM((size - 1,) + block, jnp.float32),
            pltpu.SemaphoreType.DMA((size - 1,)),
            pltpu.SemaphoreType.DMA((size - 1,)),
            pltpu.SemaphoreType.DMA((2,)),
        ],
        compiler_params=pltpu.CompilerParams(collective_id=1, has_side_effects=True),
    )(spectrum)


def per_device(visibility_real, visibility_imag, weights, labels, owner_of):
    row_count, times, channels = visibility_real.shape
    owners = lax.axis_size("bl")
    parts = lax.axis_size("tm")
    groups = owner_of.shape[0]
    per_owner = groups // owners
    capacity = 3 * row_count // (2 * owners)
    distinct = min(capacity // 4, per_owner // 2)
    row_slot, slot_rank = slots(labels, owner_of, owners, distinct)

    sent = distinct * times
    slot_id = jnp.arange(owners * sent, dtype=jnp.int32)[:, None]
    row_key = row_slot[:, None] * times + jnp.arange(times, dtype=jnp.int32)[None, :]
    row_key = row_key.reshape(1, row_count * times)
    row_weight = weights.astype(jnp.float32).reshape(1, row_count * times)
    folder = jnp.where(slot_id == row_key, row_weight, 0.0)
    part_weight = jnp.sum(folder, axis=1)
    folder = folder.astype(jnp.bfloat16)
    part_real = jnp.dot(
        folder,
        visibility_real.reshape(row_count * times, channels),
        preferred_element_type=jnp.float32,
    )
    part_imag = jnp.dot(
        folder,
        visibility_imag.reshape(row_count * times, channels),
        preferred_element_type=jnp.float32,
    )
    peak = jnp.maximum(
        jnp.max(jnp.abs(part_real), axis=1), jnp.max(jnp.abs(part_imag), axis=1)
    )
    step = lax.reduce_precision(jnp.maximum(peak, 1e-30) * (1.0078125 / 32767.0), 8, 7)
    invert = (1.0 / step)[:, None]
    code_real = jnp.round(part_real * invert).astype(jnp.int32)
    code_imag = jnp.round(part_imag * invert).astype(jnp.int32)
    packed = ((code_real << 16) | (code_imag & 65535)).reshape(owners, sent, channels)
    rank_row = jnp.broadcast_to(slot_rank[:, :, None], (owners, distinct, times))
    note = jnp.stack(
        [
            step.reshape(owners, sent),
            part_weight.reshape(owners, sent),
            rank_row.reshape(owners, sent).astype(jnp.float32),
        ],
        axis=1,
    )
    note = jnp.pad(note, ((0, 0), (0, 5), (0, -sent % 128)))
    came, came_note = exchange(packed, note)
    came_note = came_note[:, :, :sent]

    came_step = came_note[:, 0].reshape(1, owners * sent)
    came_weight = came_note[:, 1].reshape(1, owners * sent)
    came_rank = came_note[:, 2].reshape(1, owners * sent).astype(jnp.int32)
    came_time = jnp.arange(owners * sent, dtype=jnp.int32)[None, :] % times
    item = jnp.arange(times * per_owner, dtype=jnp.int32)[:, None]
    chosen = item == came_time * per_owner + came_rank
    selector = jnp.where(chosen, came_step, 0.0).astype(jnp.bfloat16)
    weight_sum = jnp.sum(jnp.where(chosen, came_weight, 0.0), axis=1)
    scale = (1.0 / jnp.maximum(weight_sum, 1.0)).reshape(times * per_owner, 1)

    came = came.reshape(owners * sent, channels)
    real_high = (came >> 24).astype(jnp.bfloat16)
    real_low = ((came >> 16) & 255).astype(jnp.bfloat16)
    imag_code = (came << 16) >> 16
    imag_high = (imag_code >> 8).astype(jnp.bfloat16)
    imag_low = (imag_code & 255).astype(jnp.bfloat16)

    def gather(high, low):
        upper = jnp.dot(selector, high, preferred_element_type=jnp.float32)
        lower = jnp.dot(selector, low, preferred_element_type=jnp.float32)
        return 256.0 * upper + lower

    taper = taper_of(channels)[None, :]
    mean_real = gather(real_high, real_low) * scale * taper
    mean_imag = gather(imag_high, imag_low) * scale * taper
    short = channels // RADIX
    r = [mean_real[:, i * short : (i + 1) * short] for i in range(RADIX)]
    m = [mean_imag[:, i * short : (i + 1) * short] for i in range(RADIX)]
    er, ei, fr, fi = r[0] + r[2], m[0] + m[2], r[1] + r[3], m[1] + m[3]
    gr, gi, hr, hi = r[0] - r[2], m[0] - m[2], r[1] - r[3], m[1] - m[3]
    folded = jnp.stack(
        [
            jnp.concatenate([er + fr, ei + fi], axis=1),
            jnp.concatenate([gr + hi, gi - hr], axis=1),
            jnp.concatenate([er - fr, ei - fi], axis=1),
            jnp.concatenate([gr - hi, gi + hr], axis=1),
        ]
    )
    spectrum = jnp.einsum(
        "qnf,qfk->qnk", folded, dft_table(channels), precision=lax.Precision.HIGH
    ).reshape(RADIX, times, per_owner, 2 * short)
    total = tail(spectrum, parts)
    return total.transpose(1, 2, 0).reshape(per_owner // parts, channels)


def solution(mesh):
    placed = (P("bl", "tm", None), P("bl", "tm", None), P("bl", "tm"), P("bl"), P())
    return jax.shard_map(
        per_device, mesh=mesh, in_specs=placed, out_specs=P(("bl", "tm"), None), check_vma=False
    )
```
